32 devices in a mesh: seq: 8 (over z, y), head: 4 (over x, core).
Axes of the slice: x: 2, y: 2, z: 4, core: 2. Of those that a mesh axis runs over, the one named last changes fastest.
Arguments:
- queries: bfloat16 [4096, 512], P('seq', 'head'), may hold values from -4.5 to 4.5
- keys: bfloat16 [4096, 512], P('seq', 'head'), may hold values from -4.5 to 4.5
- values: bfloat16 [4096, 512], P('seq', 'head'), may hold values from -6 to 6
- grad_out: bfloat16 [4096, 512], P('seq', 'head'), may hold values from -6 to 6
- block_perm: int32 [4, 8], P('head'), may hold values from 0 to 7, as said below
Outputs:
- attended: bfloat16 [4096, 512], P('seq', 'head')
- grad_queries: bfloat16 [4096, 512], P('seq', 'head')
- grad_keys: bfloat16 [4096, 512], P('seq', 'head')
- grad_values: bfloat16 [4096, 512], P('seq', 'head')
The draws below stay inside these ranges and needn't reach their ends.
Inputs may be any that keep to these rules, and one draw needn't show every extreme that they name: Each row of block_perm is a permutation of 0 to 7.
All inputs are finite; a program needn't handle non-finite values.
Results may differ from the reference program's by a relative error of at most 0.007.
Values may be sent and summed in bfloat16 or wider, within the bound.
No kernel may reach another device: no remote copies, remote signals or barrier semaphores. Data moves between devices by JAX's collectives and lax.ppermute only.
A program may use at most 64 MiB of HBM per device.

```python
import jax
import jax.numpy as jnp
from jax import lax

BLK = 512
DH = 128
SEQ = 4096
NBLK = 8
HEADS = 4
D = 512


def pair_fields(key):
    base = jax.random.fold_in(key, 11)
    key_q, key_k = jax.random.split(base, 2)
    query_field = jnp.clip(jax.random.normal(key_q, (SEQ, D), jnp.float32), -4.5, 4.5)
    key_field = jnp.clip(jax.random.normal(key_k, (SEQ, D), jnp.float32), -4.5, 4.5)
    return (query_field, key_field)


def draw_queries(key, part):
    return pair_fields(key)[0].astype(jnp.bfloat16)


def draw_keys(key, part):
    return pair_fields(key)[1].astype(jnp.bfloat16)


def draw_block_perm(key, part):
    base = jax.random.fold_in(key, 5)
    raw = jax.random.randint(base, (HEADS, NBLK), 0, 1 << 20)
    distinct = raw * NBLK + jnp.arange(NBLK, dtype=jnp.int32)[None, :]
    return jnp.argsort(distinct, axis=1, stable=True).astype(jnp.int32)


def steps_of(own_key, dims, shards, least, top_value):
    loudness = 1.0
    for position, parts in shards:
        heights = jax.random.uniform(jax.random.fold_in(jax.random.fold_in(own_key, 6), position), (parts,), jnp.float32, least / len(shards), top_value / len(shards))
        loudness = loudness * jnp.repeat(jnp.exp(heights), dims[position] // parts).reshape((-1,) + (1,) * (len(dims) - 1 - position))
    return loudness


def normal_values(own_key, dims, deviation, most, cuts=(), held_as=jnp.bfloat16):
    drawn = jax.random.normal(own_key, dims, jnp.float32) * deviation
    if len(cuts) > 0:
        drawn = steps_of(own_key, dims, cuts, -0.22, 0.18) * drawn
    return jnp.clip(drawn, min=-most, max=most).astype(held_as)


def setup_inputs(seed: int = 0) -> dict:
    key_of = jax.random.split(jax.random.key(seed), 6)
    queries = draw_queries(jax.random.fold_in(key_of[5], 71), 0)
    keys = draw_keys(jax.random.fold_in(key_of[5], 71), 0)
    values = normal_values(key_of[2], (SEQ, D), 1.0, 6.0, ((0, 8), (1, 4)))
    grad_out = normal_values(key_of[3], (SEQ, D), 1.0, 6.0, ((0, 8), (1, 4)))
    block_perm = draw_block_perm(jax.random.fold_in(key_of[5], 71), 0)
    return dict(queries=queries, keys=keys, values=values, grad_out=grad_out, block_perm=block_perm)


def window_block(query_rows, window, grad_rows, has_prev):
    width = query_rows.shape[1]
    span = query_rows.shape[0]
    scale = width ** -0.5
    win_keys = window[:, :width]
    win_values = window[:, width:]
    scores = jnp.dot(query_rows, win_keys.T, preferred_element_type=jnp.float32) * scale
    column = jnp.arange(window.shape[0], dtype=jnp.int32)
    allowed = jnp.logical_or(column >= span, has_prev)
    scores = jnp.where(allowed[None, :], scores, -1e30)
    top = jnp.max(scores, axis=1, keepdims=True)
    expon = jnp.exp(scores - top)
    probs = expon / jnp.sum(expon, axis=1, keepdims=True)
    probs_low = probs.astype(jnp.bfloat16)
    attended = jnp.dot(probs_low, win_values, preferred_element_type=jnp.float32).astype(jnp.bfloat16)
    grad_probs = jnp.dot(grad_rows, win_values.T, preferred_element_type=jnp.float32)
    delta = jnp.sum(probs * grad_probs, axis=1, keepdims=True)
    grad_scores = (probs * (grad_probs - delta) * scale).astype(jnp.bfloat16)
    grad_query = jnp.dot(grad_scores, win_keys, preferred_element_type=jnp.float32).astype(jnp.bfloat16)
    grad_key = jnp.dot(grad_scores.T, query_rows, preferred_element_type=jnp.float32)
    grad_value = jnp.dot(probs_low.T, grad_rows, preferred_element_type=jnp.float32)
    window_grads = jnp.concatenate([grad_key, grad_value], axis=1).astype(jnp.bfloat16)
    return attended, grad_query, window_grads


def head_pass(operands):
    query_head, key_head, value_head, grad_head, perm_row = operands
    pair = jnp.concatenate([key_head, value_head], axis=2)
    zero_block = jnp.zeros((1, BLK, 2 * DH), jnp.bfloat16)
    previous = jnp.concatenate([zero_block, pair[:-1]], axis=0)
    far_pair = jnp.take(pair, perm_row, axis=0)
    windows = jnp.concatenate([previous, pair, far_pair], axis=1)
    has_prev = jnp.arange(NBLK, dtype=jnp.int32) > 0

    def one_block(items):
        return window_block(items[0], items[1], items[2], items[3])

    attended, grad_query, window_grads = lax.map(one_block, (query_head, windows, grad_head, has_prev))
    local_part = window_grads[:, BLK:2 * BLK].astype(jnp.float32)
    prev_part = window_grads[:, :BLK].astype(jnp.float32)
    far_part = window_grads[:, 2 * BLK:].astype(jnp.float32)
    prev_moved = jnp.concatenate([prev_part[1:], jnp.zeros((1, BLK, 2 * DH), jnp.float32)], axis=0)
    far_moved = jnp.zeros((NBLK, BLK, 2 * DH), jnp.float32).at[perm_row].set(far_part)
    total = (local_part + prev_moved + far_moved).astype(jnp.bfloat16)
    return attended, grad_query, total[:, :, :DH], total[:, :, DH:]


def split_heads(array):
    return array.reshape(NBLK, BLK, HEADS, DH).transpose(2, 0, 1, 3)


def join_heads(array):
    return array.transpose(1, 2, 0, 3).reshape(SEQ, D)


def reference(queries, keys, values, grad_out, block_perm):
    results = lax.map(head_pass, (split_heads(queries), split_heads(keys), split_heads(values), split_heads(grad_out), block_perm))
    return (join_heads(results[0]), join_heads(results[1]), join_heads(results[2]), join_heads(results[3]))
```

```python
import jax
import jax.numpy as jnp
from jax import lax
from jax.sharding import PartitionSpec as P

BLK = 512


def passed_along(value, axis, steps):
    count = lax.axis_size(axis)
    first, last = (max(0, -steps), min(count, count - steps))
    return lax.ppermute(value, axis, [(source, source + steps) for source in range(first, last)])


def window_block(query_rows, window, grad_rows, has_prev):
    width = query_rows.shape[1]
    span = query_rows.shape[0]
    scale = width ** (-0.5)
    win_keys = window[:, :width]
    win_values = window[:, width:]
    scores = jnp.dot(query_rows, win_keys.T, preferred_element_type=jnp.float32) * scale
    column = jnp.arange(window.shape[0], dtype=jnp.int32)
    allowed = jnp.logical_or(column >= span, has_prev)
    scores = jnp.where(allowed[None, :], scores, -1e30)
    top = jnp.max(scores, axis=1, keepdims=True)
    expon = jnp.exp(scores - top)
    probs = expon / jnp.sum(expon, axis=1, keepdims=True)
    probs_low = probs.astype(jnp.bfloat16)
    attended = jnp.dot(probs_low, win_values, preferred_element_type=jnp.float32).astype(
        jnp.bfloat16
    )
    grad_probs = jnp.dot(grad_rows, win_values.T, preferred_element_type=jnp.float32)
    delta = jnp.sum(probs * grad_probs, axis=1, keepdims=True)
    grad_scores = (probs * (grad_probs - delta) * scale).astype(jnp.bfloat16)
    grad_query = jnp.dot(grad_scores, win_keys, preferred_element_type=jnp.float32).astype(
        jnp.bfloat16
    )
    grad_key = jnp.dot(grad_scores.T, query_rows, preferred_element_type=jnp.float32)
    grad_value = jnp.dot(probs_low.T, grad_rows, preferred_element_type=jnp.float32)
    window_grads = jnp.concatenate([grad_key, grad_value], axis=1).astype(jnp.bfloat16)
    return (attended, grad_query, window_grads)


def routed(blocks, order):
    here, rows, width = blocks.shape
    count = lax.axis_size("seq")
    part = rows // count
    cut = blocks.reshape(here, count, part, width).transpose(1, 0, 2, 3)
    spread = lax.all_to_all(cut, "seq", 0, 0)
    sorted_slices = jnp.take(spread.reshape(count * here, part, width), order, axis=0)
    back = lax.all_to_all(sorted_slices.reshape(count, here, part, width), "seq", 0, 0)
    return back.transpose(1, 0, 2, 3).reshape(here, rows, width)


def body(queries, keys, values, grad_out, block_perm):
    width = queries.shape[1]
    blocks_here = queries.shape[0] // BLK
    seq_index = lax.axis_index("seq")
    query_blocks = queries.reshape(blocks_here, BLK, width)
    grad_blocks = grad_out.reshape(blocks_here, BLK, width)
    pair = jnp.concatenate(
        [keys.reshape(blocks_here, BLK, width), values.reshape(blocks_here, BLK, width)], axis=2
    )
    order = block_perm[0]
    inverse = jnp.argmax(
        order[None, :] == jnp.arange(order.shape[0], dtype=jnp.int32)[:, None], axis=1
    )
    prev_pair = passed_along(pair[blocks_here - 1], "seq", 1)
    far_pair = routed(pair, order)
    previous = jnp.concatenate([prev_pair[None], pair[:-1]], axis=0)
    windows = jnp.concatenate([previous, pair, far_pair], axis=1)
    has_prev = seq_index * blocks_here + jnp.arange(blocks_here, dtype=jnp.int32) > 0

    def one_block(items):
        return window_block(items[0], items[1], items[2], items[3])

    attended, grad_query, window_grads = lax.map(
        one_block, (query_blocks, windows, grad_blocks, has_prev)
    )
    prev_back = passed_along(window_grads[0, :BLK], "seq", -1)
    far_back = routed(window_grads[:, 2 * BLK :], inverse)
    local_part = window_grads[:, BLK : 2 * BLK].astype(jnp.float32)
    prev_moved = jnp.concatenate([window_grads[1:, :BLK], prev_back[None]], axis=0).astype(
        jnp.float32
    )
    far_moved = far_back.astype(jnp.float32)
    total = (
        (local_part + prev_moved + far_moved)
        .astype(jnp.bfloat16)
        .reshape(blocks_here * BLK, 2 * width)
    )
    return (
        attended.reshape(blocks_here * BLK, width),
        grad_query.reshape(blocks_here * BLK, width),
        total[:, :width],
        total[:, width:],
    )


def solution(mesh):
    placed = (
        P("seq", "head"),
        P("seq", "head"),
        P("seq", "head"),
        P("seq", "head"),
        P("head", None),
    )
    return jax.shard_map(
        body,
        mesh=mesh,
        in_specs=placed,
        out_specs=(P("seq", "head"), P("seq", "head"), P("seq", "head"), P("seq", "head")),
        check_vma=False,
    )
```

```python
import jax
import jax.numpy as jnp
from jax import lax
from jax.experimental import pallas as pl
from jax.experimental.pallas import tpu as pltpu
from jax.sharding import PartitionSpec as P


NEVER = -1e30
NOTE_ROWS = 16
FEW = 8


def passed_along(value, axis, steps):
    count = lax.axis_size(axis)
    first, last = (max(0, -steps), min(count, count - steps))
    return lax.ppermute(value, axis, [(source, source + steps) for source in range(first, last)])


def rows_by_rows(left, right):
    return lax.dot_general(
        left, right, (((1,), (1,)), ((), ())), preferred_element_type=jnp.float32
    )


def times(left, right):
    return jnp.dot(left, right, preferred_element_type=jnp.float32)


def chunks(rows, size):
    return [(place, pl.ds(place * size, size)) for place in range(rows // size)]


def pack_lent(key, value, joint, slices):
    width = key.shape[1]
    for side, array in enumerate((key, value)):
        lanes = slice(side * width, (side + 1) * width)
        joint[:, lanes] = array[...]
        slices[:, :, lanes] = array[...].reshape(slices.shape[0], slices.shape[1], width)


def split_asked(place, query, grad, joint, kept, sent):
    _, width = query.shape
    half, part, _ = kept.shape
    joint[:, :width] = query[...]
    joint[:, width:] = grad[...]
    for step in range(half):
        for flip, out in enumerate((kept, sent)):
            target = 2 * step + ((place[0] & 1) ^ flip)
            start = pl.multiple_of(target * part, part)
            out[step, :, :width] = query[pl.ds(start, part), :]
            out[step, :, width:] = grad[pl.ds(start, part), :]


def regroup(place, kept, got, *outs):
    for step, out in enumerate(outs):
        source = (place[0] // 2) ^ step
        out[0] = kept[source]
        out[1] = got[source]


def near_statistics(place, query, grad, key, value, previous, level_out, delta_out):
    rows, width = query.shape
    scale = width ** (-0.5)
    has_prev = place[0] > 0
    for _, cut in chunks(rows, 2 * width):
        scores = rows_by_rows(key[...], query[cut, :]) * scale
        prev_scores = rows_by_rows(previous[:, :width], query[cut, :]) * scale
        prev_scores = jnp.where(has_prev, prev_scores, NEVER)
        top = jnp.maximum(
            jnp.max(scores, axis=0, keepdims=True), jnp.max(prev_scores, axis=0, keepdims=True)
        )
        expon = jnp.exp(scores - top)
        prev_expon = jnp.exp(prev_scores - top)
        grad_probs = rows_by_rows(value[...], grad[cut, :])
        prev_grad_probs = rows_by_rows(previous[:, width:], grad[cut, :])
        mass = jnp.sum(expon + prev_expon, axis=0, keepdims=True)
        mixed = jnp.sum(
            expon * grad_probs + prev_expon * prev_grad_probs, axis=0, keepdims=True
        )
        level_out[:, cut] = top + jnp.log(mass)
        delta_out[:, cut] = mixed / mass


def pick_lent(perm, slices, out):
    for target in range(out.shape[0]):
        out[target] = slices[perm[0, target]]


def noted(lines, note, double):
    note[...] = jnp.zeros(note.shape, note.dtype)
    row = 0
    for source, pieces in ((0, 3), (1, 2)):
        values = lines[source : source + 1, :]
        for _ in range(pieces):
            head = values.astype(jnp.bfloat16).astype(jnp.float32)
            values = values - head
            for line in range(values.shape[1] // double):
                note[row : row + 1, :] = head[:, line * double : (line + 1) * double]
                row += 1
    return note[...].astype(jnp.bfloat16)


def pick_asked(place, perm, lines, *arrays):
    half = len(arrays) - 3
    out, scratch, note = arrays[half:]
    part = scratch.shape[1]
    pieces = noted(lines, note, scratch.shape[2])
    for step in range(half):
        scratch[2 * step] = arrays[step][0]
        scratch[2 * step + 1] = arrays[step][1]
    for block in range(2 * half):
        out[perm[0, block], :part, :] = scratch[place[0] ^ block]
        out[block, part:, :] = pieces


def pick_asked_stacked(perm, lines, slices, out, note):
    count, part, double = slices.shape
    pieces = noted(lines, note, double)
    for block in range(count):
        out[perm[0, block], :part, :] = slices[block]
        out[block, part:, :] = pieces


def fetched(brought, rows):
    count, _, double = brought.shape
    part = rows // count
    width = double // 2
    return (
        brought[:, :part, :width].reshape(rows, width),
        brought[:, :part, width:].reshape(rows, width),
    )


def merged(scores, grad_probs, near_level, near_delta):
    top = jnp.maximum(jnp.max(scores, axis=0, keepdims=True), near_level)
    expon = jnp.exp(scores - top)
    kept = jnp.exp(near_level - top)
    mass = kept + jnp.sum(expon, axis=0, keepdims=True)
    mixed = near_delta * kept + jnp.sum(expon * grad_probs, axis=0, keepdims=True)
    share = 1.0 / mass
    return top, expon, mass, share, mixed * share


def far_statistics(query, grad, brought, near_level, near_delta, lines):
    rows, width = query.shape
    scale = width ** (-0.5)
    far_key, far_value = fetched(brought, rows)
    for _, cut in chunks(rows, 2 * width):
        scores = rows_by_rows(far_key, query[cut, :]) * scale
        grad_probs = rows_by_rows(far_value, grad[cut, :])
        top, _, mass, _, delta = merged(scores, grad_probs, near_level[:, cut], near_delta[:, cut])
        lines[0:1, cut] = top + jnp.log(mass)
        lines[1:2, cut] = delta


def query_side(
    place, query, grad, key, value, previous, brought, lines, attended, grad_query, own_grads
):
    rows, width = query.shape
    scale = width ** (-0.5)
    has_prev = place[0] > 0
    sides = (
        (previous[:, :width], previous[:, width:]),
        (key[...], value[...]),
        fetched(brought, rows),
    )
    turned = [(keys.T, values.T) for keys, values in sides]
    grad_key = 0.0
    grad_value = 0.0
    for _, cut in chunks(rows, 2 * width):
        out_turned = 0.0
        grad_turned = 0.0
        for side, (keys, values) in enumerate(sides):
            scores = rows_by_rows(keys, query[cut, :]) * scale
            if side == 0:
                scores = jnp.where(has_prev, scores, NEVER)
            grad_probs = rows_by_rows(values, grad[cut, :])
            probs = jnp.exp(scores - lines[0:1, cut])
            grad_scores = (probs * (grad_probs - lines[1:2, cut])).astype(jnp.bfloat16)
            probs_low = probs.astype(jnp.bfloat16)
            out_turned += times(turned[side][1], probs_low)
            grad_turned += times(turned[side][0], grad_scores)
            if side == 1:
                grad_key += times(grad_scores, query[cut, :])
                grad_value += times(probs_low, grad[cut, :])
        attended[cut, :] = out_turned.T.astype(attended.dtype)
        grad_query[cut, :] = (grad_turned * scale).T.astype(grad_query.dtype)
    own_grads[:, :width] = grad_key * scale
    own_grads[:, width:] = grad_value


def next_asking(place, perm, key, value, asking, lines, own_grads, sums):
    rows, width = key.shape
    scale = width ** (-0.5)
    allowed = place[0] + 1 < perm.shape[1]
    grad_key = 0.0
    grad_value = 0.0
    for _, cut in chunks(rows, 2 * width):
        scores = rows_by_rows(key[...], asking[cut, :width]) * scale
        scores = jnp.where(allowed, scores, NEVER)
        grad_probs = rows_by_rows(value[...], asking[cut, width:])
        probs = jnp.exp(scores - lines[0:1, cut])
        grad_scores = (probs * (grad_probs - lines[1:2, cut])).astype(jnp.bfloat16)
        grad_key += times(grad_scores, asking[cut, :width])
        grad_value += times(probs.astype(jnp.bfloat16), asking[cut, width:])
    sums[:, :width] = own_grads[:, :width] + grad_key * scale
    sums[:, width:] = own_grads[:, width:] + grad_value


def far_asking(place, perm, key, value, asked, sums, key_out, value_out):
    rows, width = key.shape
    scale = width ** (-0.5)
    count = asked.shape[0]
    asker = jnp.int32(0)
    for block in range(count):
        asker = jnp.where(perm[0, block] == place[0], jnp.int32(block), asker)
    note = asked[asker, rows // count :, :].astype(jnp.float32)
    lines = rows // (2 * width)
    query, grad = fetched(asked, rows)
    grad_key = 0.0
    grad_value = 0.0
    for line, _ in chunks(rows, 2 * width):
        pieces = [note[line + lines * piece][None] for piece in range(5)]
        inside = slice(line * 2 * width, (line + 1) * 2 * width)
        scores = rows_by_rows(key[...], query[inside]) * scale
        grad_probs = rows_by_rows(value[...], grad[inside])
        probs = jnp.exp(scores - (pieces[0] + pieces[1] + pieces[2]))
        grad_scores = (probs * (grad_probs - (pieces[3] + pieces[4]))).astype(jnp.bfloat16)
        grad_key += times(grad_scores, query[inside])
        grad_value += times(probs.astype(jnp.bfloat16), grad[inside])
    key_out[...] = (sums[:, :width] + grad_key * scale).astype(key_out.dtype)
    value_out[...] = (sums[:, width:] + grad_value).astype(value_out.dtype)


VMEM = pl.BlockSpec(memory_space=pltpu.VMEM)
SMEM = pl.BlockSpec(memory_space=pltpu.SMEM)


def on_chip(array):
    return pltpu.with_memory_space_constraint(array, pltpu.VMEM)


def call(kernel, outs, *operands, scalars=0, leaving=(), scratch=(), free=False):
    return pl.pallas_call(
        kernel,
        out_shape=tuple(
            jax.ShapeDtypeStruct(shape, dtype) if place in leaving else pltpu.VMEM(shape, dtype)
            for place, (shape, dtype) in enumerate(outs)
        ),
        in_specs=[SMEM] * scalars + [VMEM] * (len(operands) - scalars),
        out_specs=tuple(VMEM for _ in outs),
        scratch_shapes=scratch,
    )(*operands[:scalars], *(operand if free else on_chip(operand) for operand in operands[scalars:]))


def exchanged(cut):
    return lax.all_to_all(cut, "seq", 0, 0)


def layer(query, key, value, grad, perm):
    rows, width = query.shape
    count = lax.axis_size("seq")
    part = rows // count
    place = lax.axis_index("seq").astype(jnp.int32)
    low = jnp.bfloat16
    place = place.reshape(1)
    row = ((1, rows), jnp.float32)
    double = ((rows, 2 * width), jnp.float32)
    half = ((rows, width), low)
    cut = ((count, part, 2 * width), low)
    lent, packed = call(pack_lent, ((double[0], low), cut), key, value, leaving=(1,), free=True)
    lent_before = passed_along(lent, "seq", 1)
    lent_slices = exchanged(packed)
    if count <= FEW:
        quarter = ((count // 2, part, 2 * width), low)
        asked, kept, sent = call(
            split_asked, ((double[0], low), quarter, quarter), place, query, grad, scalars=1
        )
        got = lax.ppermute(sent, "seq", [(source, source ^ 1) for source in range(count)])
        asked_parts = list(
            call(
                regroup,
                (((2, part, 2 * width), low),) * (count // 2),
                place,
                kept,
                got,
                scalars=1,
            )
        )
        for step in range(1, count // 2):
            asked_parts[step] = lax.ppermute(
                asked_parts[step],
                "seq",
                [(source, source ^ (2 * step)) for source in range(count)],
            )
    else:
        asked = jnp.concatenate([query, grad], axis=1)
        asked_slices = exchanged(asked.reshape(cut[0]))
    asked_after = passed_along(asked, "seq", -1)
    near = call(near_statistics, (row, row), place, query, grad, key, value, lent_before, scalars=1)
    lent_sorted = call(pick_lent, (cut,), perm, lent_slices, scalars=1, leaving=(0,))[0]
    brought = exchanged(lent_sorted)
    lines = call(
        far_statistics, (((2, rows), jnp.float32),), query, grad, brought, *near
    )[0]
    noting = ((count, part + NOTE_ROWS, 2 * width), low)
    note = pltpu.VMEM((NOTE_ROWS, 2 * width), jnp.float32)
    if count <= FEW:
        asked_sorted = call(
            pick_asked,
            (noting,),
            place,
            perm,
            lines,
            *asked_parts,
            scalars=2,
            leaving=(0,),
            scratch=[pltpu.VMEM(*cut), note],
        )[0]
    else:
        asked_sorted = call(
            pick_asked_stacked,
            (noting,),
            perm,
            lines,
            asked_slices,
            scalars=1,
            leaving=(0,),
            scratch=[note],
        )[0]
    far_asked = exchanged(asked_sorted)
    lines_after = passed_along(lines, "seq", -1)
    attended, grad_query, own_grads = call(
        query_side,
        (half, half, double),
        place,
        query,
        grad,
        key,
        value,
        lent_before,
        brought,
        lines,
        scalars=1,
        leaving=(0, 1),
    )
    sums = call(
        next_asking,
        (double,),
        place,
        perm,
        key,
        value,
        asked_after,
        lines_after,
        own_grads,
        scalars=2,
    )[0]
    grad_key, grad_value = call(
        far_asking,
        (half, half),
        place,
        perm,
        key,
        value,
        far_asked,
        sums,
        scalars=2,
        leaving=(0, 1),
    )
    return attended, grad_query, grad_key, grad_value


def solution(mesh):
    placed = (
        P("seq", "head"),
        P("seq", "head"),
        P("seq", "head"),
        P("seq", "head"),
        P("head", None),
    )
    return jax.shard_map(
        layer,
        mesh=mesh,
        in_specs=placed,
        out_specs=(P("seq", "head"), P("seq", "head"), P("seq", "head"), P("seq", "head")),
        check_vma=False,
    )
```

```python
import jax
import jax.numpy as jnp
from jax import lax
from jax.experimental import pallas as pl
from jax.experimental.pallas import tpu as pltpu
from jax.sharding import PartitionSpec as P


NEVER = -1e30
NOTE_ROWS = 8
FEW = 8


def passed_along(value, axis, steps):
    count = lax.axis_size(axis)
    first, last = (max(0, -steps), min(count, count - steps))
    return lax.ppermute(value, axis, [(source, source + steps) for source in range(first, last)])


def rows_by_rows(left, right):
    return lax.dot_general(
        left, right, (((1,), (1,)), ((), ())), preferred_element_type=jnp.float32
    )


def times(left, right):
    return jnp.dot(left, right, preferred_element_type=jnp.float32)


def chunks(rows, size):
    return [(place, pl.ds(place * size, size)) for place in range(rows // size)]


def pack_lent(key, value, joint, slices):
    width = key.shape[1]
    for side, array in enumerate((key, value)):
        lanes = slice(side * width, (side + 1) * width)
        joint[:, lanes] = array[...]
        slices[:, :, lanes] = array[...].reshape(slices.shape[0], slices.shape[1], width)


def split_asked(place, query, grad, joint, kept, sent):
    _, width = query.shape
    half, part, _ = kept.shape
    joint[:, :width] = query[...]
    joint[:, width:] = grad[...]
    for step in range(half):
        for flip, out in enumerate((kept, sent)):
            target = step + half * ((place[0] // half) ^ flip)
            start = pl.multiple_of(target * part, part)
            out[step, :, :width] = query[pl.ds(start, part), :]
            out[step, :, width:] = grad[pl.ds(start, part), :]


def regroup(place, kept, got, *outs):
    for step, out in enumerate(outs):
        source = (place[0] % len(outs)) ^ step
        out[0] = kept[source]
        out[1] = got[source]


def near_statistics(place, query, grad, key, value, previous, level_out, delta_out):
    rows, width = query.shape
    scale = width ** (-0.5)
    has_prev = place[0] > 0
    for _, cut in chunks(rows, 2 * width):
        scores = rows_by_rows(key[...], query[cut, :]) * scale
        prev_scores = rows_by_rows(previous[:, :width], query[cut, :]) * scale
        prev_scores = jnp.where(has_prev, prev_scores, NEVER)
        top = jnp.maximum(
            jnp.max(scores, axis=0, keepdims=True), jnp.max(prev_scores, axis=0, keepdims=True)
        )
        expon = jnp.exp(scores - top)
        prev_expon = jnp.exp(prev_scores - top)
        grad_probs = rows_by_rows(value[...], grad[cut, :])
        prev_grad_probs = rows_by_rows(previous[:, width:], grad[cut, :])
        mass = jnp.sum(expon + prev_expon, axis=0, keepdims=True)
        mixed = jnp.sum(
            expon * grad_probs + prev_expon * prev_grad_probs, axis=0, keepdims=True
        )
        level_out[:, cut] = top + jnp.log(mass)
        delta_out[:, cut] = mixed / mass


def pick_lent(perm, slices, out):
    for target in range(out.shape[0]):
        out[target] = slices[perm[0, target]]


def noted(lines, note, double):
    note[...] = jnp.zeros(note.shape, note.dtype)
    row = 0
    for source, pieces in ((0, 2), (1, 2)):
        values = lines[source : source + 1, :]
        for _ in range(pieces):
            head = values.astype(jnp.bfloat16).astype(jnp.float32)
            values = values - head
            for line in range(values.shape[1] // double):
                note[row : row + 1, :] = head[:, line * double : (line + 1) * double]
                row += 1
    return note[...].astype(jnp.bfloat16)


def pick_asked(place, perm, lines, *arrays):
    half = len(arrays) - 3
    out, scratch, note = arrays[half:]
    part = scratch.shape[1]
    pieces = noted(lines, note, scratch.shape[2])
    for step in range(half):
        scratch[step] = arrays[step][0]
        scratch[half + step] = arrays[step][1]
    for block in range(2 * half):
        out[perm[0, block], :part, :] = scratch[place[0] ^ block]
        out[block, part:, :] = pieces


def pick_asked_stacked(perm, lines, slices, out, note):
    count, part, double = slices.shape
    pieces = noted(lines, note, double)
    for block in range(count):
        out[perm[0, block], :part, :] = slices[block]
        out[block, part:, :] = pieces


def fetched(brought, rows):
    count, _, double = brought.shape
    part = rows // count
    width = double // 2
    return (
        brought[:, :part, :width].reshape(rows, width),
        brought[:, :part, width:].reshape(rows, width),
    )


def merged(scores, grad_probs, near_level, near_delta):
    top = jnp.maximum(jnp.max(scores, axis=0, keepdims=True), near_level)
    expon = jnp.exp(scores - top)
    kept = jnp.exp(near_level - top)
    mass = kept + jnp.sum(expon, axis=0, keepdims=True)
    mixed = near_delta * kept + jnp.sum(expon * grad_probs, axis=0, keepdims=True)
    share = 1.0 / mass
    return top, expon, mass, share, mixed * share


def far_statistics(query, grad, brought, near_level, near_delta, lines):
    rows, width = query.shape
    scale = width ** (-0.5)
    far_key, far_value = fetched(brought, rows)
    for _, cut in chunks(rows, 2 * width):
        scores = rows_by_rows(far_key, query[cut, :]) * scale
        grad_probs = rows_by_rows(far_value, grad[cut, :])
        top, _, mass, _, delta = merged(scores, grad_probs, near_level[:, cut], near_delta[:, cut])
        lines[0:1, cut] = top + jnp.log(mass)
        lines[1:2, cut] = delta


def query_side(
    place, query, grad, key, value, previous, brought, lines, attended, grad_query, own_grads
):
    rows, width = query.shape
    scale = width ** (-0.5)
    has_prev = place[0] > 0
    sides = (
        (previous[:, :width], previous[:, width:]),
        (key[...], value[...]),
        fetched(brought, rows),
    )
    turned = [(keys.T, values.T) for keys, values in sides]
    grad_key = 0.0
    grad_value = 0.0
    for _, cut in chunks(rows, 2 * width):
        out_turned = 0.0
        grad_turned = 0.0
        for side, (keys, values) in enumerate(sides):
            scores = rows_by_rows(keys, query[cut, :]) * scale
            if side == 0:
                scores = jnp.where(has_prev, scores, NEVER)
            grad_probs = rows_by_rows(values, grad[cut, :])
            probs = jnp.exp(scores - lines[0:1, cut])
            grad_scores = (probs * (grad_probs - lines[1:2, cut])).astype(jnp.bfloat16)
            probs_low = probs.astype(jnp.bfloat16)
            out_turned += times(turned[side][1], probs_low)
            grad_turned += times(turned[side][0], grad_scores)
            if side == 1:
                grad_key += times(grad_scores, query[cut, :])
                grad_value += times(probs_low, grad[cut, :])
        attended[cut, :] = out_turned.T.astype(attended.dtype)
        grad_query[cut, :] = (grad_turned * scale).T.astype(grad_query.dtype)
    own_grads[:, :width] = grad_key * scale
    own_grads[:, width:] = grad_value


def next_asking(place, perm, key, value, asking, lines, own_grads, sums):
    rows, width = key.shape
    scale = width ** (-0.5)
    allowed = place[0] + 1 < perm.shape[1]
    grad_key = 0.0
    grad_value = 0.0
    for _, cut in chunks(rows, 2 * width):
        scores = rows_by_rows(key[...], asking[cut, :width]) * scale
        scores = jnp.where(allowed, scores, NEVER)
        grad_probs = rows_by_rows(value[...], asking[cut, width:])
        probs = jnp.exp(scores - lines[0:1, cut])
        grad_scores = (probs * (grad_probs - lines[1:2, cut])).astype(jnp.bfloat16)
        grad_key += times(grad_scores, asking[cut, :width])
        grad_value += times(probs.astype(jnp.bfloat16), asking[cut, width:])
    sums[:, :width] = own_grads[:, :width] + grad_key * scale
    sums[:, width:] = own_grads[:, width:] + grad_value


def far_asking(place, perm, key, value, asked, sums, key_out, value_out):
    rows, width = key.shape
    scale = width ** (-0.5)
    count = asked.shape[0]
    asker = jnp.int32(0)
    for block in range(count):
        asker = jnp.where(perm[0, block] == place[0], jnp.int32(block), asker)
    note = asked[asker, rows // count :, :].astype(jnp.float32)
    lines = rows // (2 * width)
    query, grad = fetched(asked, rows)
    grad_key = 0.0
    grad_value = 0.0
    for line, _ in chunks(rows, 2 * width):
        pieces = [note[line + lines * piece][None] for piece in range(4)]
        inside = slice(line * 2 * width, (line + 1) * 2 * width)
        scores = rows_by_rows(key[...], query[inside]) * scale
        grad_probs = rows_by_rows(value[...], grad[inside])
        probs = jnp.exp(scores - (pieces[0] + pieces[1]))
        grad_scores = (probs * (grad_probs - (pieces[2] + pieces[3]))).astype(jnp.bfloat16)
        grad_key += times(grad_scores, query[inside])
        grad_value += times(probs.astype(jnp.bfloat16), grad[inside])
    key_out[...] = (sums[:, :width] + grad_key * scale).astype(key_out.dtype)
    value_out[...] = (sums[:, width:] + grad_value).astype(value_out.dtype)


VMEM = pl.BlockSpec(memory_space=pltpu.VMEM)
SMEM = pl.BlockSpec(memory_space=pltpu.SMEM)


def on_chip(array):
    return pltpu.with_memory_space_constraint(array, pltpu.VMEM)


def call(kernel, outs, *operands, scalars=0, leaving=(), scratch=(), free=False):
    return pl.pallas_call(
        kernel,
        out_shape=tuple(
            jax.ShapeDtypeStruct(shape, dtype) if place in leaving else pltpu.VMEM(shape, dtype)
            for place, (shape, dtype) in enumerate(outs)
        ),
        in_specs=[SMEM] * scalars + [VMEM] * (len(operands) - scalars),
        out_specs=tuple(VMEM for _ in outs),
        scratch_shapes=scratch,
    )(*operands[:scalars], *(operand if free else on_chip(operand) for operand in operands[scalars:]))


def exchanged(cut):
    return lax.all_to_all(cut, "seq", 0, 0)


def layer(query, key, value, grad, perm):
    rows, width = query.shape
    count = lax.axis_size("seq")
    part = rows // count
    place = lax.axis_index("seq").astype(jnp.int32)
    low = jnp.bfloat16
    place = place.reshape(1)
    row = ((1, rows), jnp.float32)
    double = ((rows, 2 * width), jnp.float32)
    half = ((rows, width), low)
    cut = ((count, part, 2 * width), low)
    lent, packed = call(pack_lent, ((double[0], low), cut), key, value, leaving=(1,), free=True)
    lent_before = passed_along(lent, "seq", 1)
    lent_slices = exchanged(packed)
    if count <= FEW:
        quarter = ((count // 2, part, 2 * width), low)
        asked, kept, sent = call(
            split_asked,
            ((double[0], low), quarter, quarter),
            place,
            query,
            grad,
            scalars=1,
            free=True,
        )
        got = lax.ppermute(sent, "seq", [(source, source ^ (count // 2)) for source in range(count)])
        asked_parts = list(
            call(
                regroup,
                (((2, part, 2 * width), low),) * (count // 2),
                place,
                kept,
                got,
                scalars=1,
            )
        )
        for step in range(1, count // 2):
            asked_parts[step] = lax.ppermute(
                asked_parts[step],
                "seq",
                [(source, source ^ step) for source in range(count)],
            )
    else:
        asked = jnp.concatenate([query, grad], axis=1)
        asked_slices = exchanged(asked.reshape(cut[0]))
    asked_after = passed_along(asked, "seq", -1)
    near = call(near_statistics, (row, row), place, query, grad, key, value, lent_before, scalars=1)
    lent_sorted = call(pick_lent, (cut,), perm, lent_slices, scalars=1, leaving=(0,))[0]
    brought = exchanged(lent_sorted)
    lines = call(
        far_statistics, (((2, rows), jnp.float32),), query, grad, brought, *near
    )[0]
    noting = ((count, part + NOTE_ROWS, 2 * width), low)
    note = pltpu.VMEM((NOTE_ROWS, 2 * width), jnp.float32)
    if count <= FEW:
        asked_sorted = call(
            pick_asked,
            (noting,),
            place,
            perm,
            lines,
            *asked_parts,
            scalars=2,
            leaving=(0,),
            scratch=[pltpu.VMEM(*cut), note],
        )[0]
    else:
        asked_sorted = call(
            pick_asked_stacked,
            (noting,),
            perm,
            lines,
            asked_slices,
            scalars=1,
            leaving=(0,),
            scratch=[note],
        )[0]
    far_asked = exchanged(asked_sorted)
    lines_after = passed_along(lines, "seq", -1)
    attended, grad_query, own_grads = call(
        query_side,
        (half, half, double),
        place,
        query,
        grad,
        key,
        value,
        lent_before,
        brought,
        lines,
        scalars=1,
        leaving=(0, 1),
    )
    sums = call(
        next_asking,
        (double,),
        place,
        perm,
        key,
        value,
        asked_after,
        lines_after,
        own_grads,
        scalars=2,
    )[0]
    grad_key, grad_value = call(
        far_asking,
        (half, half),
        place,
        perm,
        key,
        value,
        far_asked,
        sums,
        scalars=2,
        leaving=(0, 1),
    )
    return attended, grad_query, grad_key, grad_value


def solution(mesh):
    placed = (
        P("seq", "head"),
        P("seq", "head"),
        P("seq", "head"),
        P("seq", "head"),
        P("head", None),
    )
    return jax.shard_map(
        layer,
        mesh=mesh,
        in_specs=placed,
        out_specs=(P("seq", "head"), P("seq", "head"), P("seq", "head"), P("seq", "head")),
        check_vma=False,
    )
```
